32 devices in a mesh: dp: 4 (over y, z), sp: 8 (over x, core).
Axes of the slice: x: 4, y: 2, z: 2, core: 2. Of those that a mesh axis runs over, the one named last changes fastest.
The devices are a block of a 4x4x8 slice.
Arguments:
- hidden: bfloat16 [8192, 2048], P(('dp', 'sp')), parts along dimension 0
- seg_ids: int32 [8192], P(('dp', 'sp')), parts along dimension 0
- norm_kv: bfloat16 [2048], replicated
- w_key: bfloat16 [2048, 32, 64], replicated
- w_value: bfloat16 [2048, 32, 64], replicated
- norm_attn: bfloat16 [1, 2048], replicated
- w_query: bfloat16 [1, 2048, 32, 64], replicated
- w_out: bfloat16 [1, 32, 64, 2048], replicated
- norm_mlp: bfloat16 [1, 2048], replicated
- w_gate: bfloat16 [1, 2048, 8192], replicated
- w_up: bfloat16 [1, 2048, 8192], replicated
- w_down: bfloat16 [1, 8192, 2048], replicated
Outputs:
- output: bfloat16 [8192, 2048], P(('dp', 'sp')), parts along dimension 0
There are 4 independent parts. The reference program is written for one: setup_inputs(seed, part) draws one part's arguments, and reference() takes and returns one part's arrays. A program takes and returns all parts, laid end to end along the dimension named above; an argument that names none is the same for every part.
All inputs are finite; a program needn't handle non-finite values.
Results may differ from the reference program's by a relative error of at most 0.0131936.
Values are sent between devices in bfloat16 or wider.
A program may use at most 768 MiB of HBM per device.

```python
import math
import jax
import jax.numpy as jnp
from jax import lax

D_MODEL = 2048
Q_HEADS = 32
KV_HEADS = 32
HEAD_DIM = 64
FF_DIM = 8192
LAYERS = 1
TOKENS_DEV = 256
SHARDS = 8
SEQ_LEN = 2048
BOUNDS = 3
Q_PER_KV = Q_HEADS // KV_HEADS
NORM_EPS = 1e-6


def rms_norm(values, gain):
    val32 = values.astype(jnp.float32)
    inv_rms = lax.rsqrt(jnp.mean(val32 * val32, axis=-1, keepdims=True) + NORM_EPS)
    return (val32 * inv_rms * gain.astype(jnp.float32)).astype(jnp.bfloat16)


def draw_seg(key):
    positions = jnp.arange(SEQ_LEN, dtype=jnp.int32)
    starts = jax.random.permutation(key, SEQ_LEN - 1)[:BOUNDS].astype(jnp.int32) + 1
    return jnp.sum((positions[:, None] >= starts[None, :]).astype(jnp.int32), axis=1).astype(jnp.int32)


def setup_inputs(seed: int = 0, part: int = 0) -> dict:
    keys = jax.random.split(jax.random.key(seed), 12)
    query_gain = max(1.5, math.sqrt(math.log(SEQ_LEN / (BOUNDS + 1))))

    def draw_normal(key, shape, scale):
        return (scale * jax.random.normal(key, shape, jnp.float32)).astype(jnp.bfloat16)

    def draw_gain(key, shape):
        return (1.0 + 0.25 * jax.random.normal(key, shape, jnp.float32)).astype(jnp.bfloat16)

    hidden = draw_normal(jax.random.fold_in(keys[0], part), (SEQ_LEN, D_MODEL), 1.0)
    seg_ids = draw_seg(jax.random.fold_in(keys[1], part))
    return {
        'hidden': hidden,
        'seg_ids': seg_ids,
        'norm_kv': draw_gain(keys[2], (D_MODEL,)),
        'w_key': draw_normal(keys[3], (D_MODEL, KV_HEADS, HEAD_DIM), D_MODEL ** -0.5),
        'w_value': draw_normal(keys[4], (D_MODEL, KV_HEADS, HEAD_DIM), D_MODEL ** -0.5),
        'norm_attn': draw_gain(keys[5], (LAYERS, D_MODEL)),
        'w_query': draw_normal(keys[6], (LAYERS, D_MODEL, Q_HEADS, HEAD_DIM), query_gain * D_MODEL ** -0.5),
        'w_out': draw_normal(keys[7], (LAYERS, Q_HEADS, HEAD_DIM, D_MODEL), (Q_HEADS * HEAD_DIM) ** -0.5),
        'norm_mlp': draw_gain(keys[8], (LAYERS, D_MODEL)),
        'w_gate': draw_normal(keys[9], (LAYERS, D_MODEL, FF_DIM), D_MODEL ** -0.5),
        'w_up': draw_normal(keys[10], (LAYERS, D_MODEL, FF_DIM), D_MODEL ** -0.5),
        'w_down': draw_normal(keys[11], (LAYERS, FF_DIM, D_MODEL), FF_DIM ** -0.5),
    }


def reference(hidden, seg_ids, norm_kv, w_key, w_value, norm_attn, w_query, w_out, norm_mlp, w_gate, w_up, w_down):
    kv_width = KV_HEADS * HEAD_DIM
    q_width = Q_HEADS * HEAD_DIM
    u_kv = rms_norm(hidden, norm_kv)
    keys = jnp.dot(u_kv, w_key.reshape(D_MODEL, kv_width), preferred_element_type=jnp.float32).astype(jnp.bfloat16)
    keys = keys.reshape(SEQ_LEN, KV_HEADS, HEAD_DIM).astype(jnp.float32)
    values = jnp.dot(u_kv, w_value.reshape(D_MODEL, kv_width), preferred_element_type=jnp.float32).astype(jnp.bfloat16)
    values = values.reshape(SEQ_LEN, KV_HEADS, HEAD_DIM).astype(jnp.float32)
    positions = jnp.arange(SEQ_LEN, dtype=jnp.int32)
    blk_pos = positions.reshape(SHARDS, TOKENS_DEV)
    blk_seg = seg_ids.reshape(SHARDS, TOKENS_DEV)
    scale = HEAD_DIM ** -0.5

    def block_attention(block):
        q_blk, q_pos, q_seg = block
        scores = jnp.einsum('qrgd,kgd->grqk', q_blk, keys) * scale
        allowed = (positions[None, :] <= q_pos[:, None]) & (seg_ids[None, :] == q_seg[:, None])
        scores = jnp.where(allowed[None, None], scores, -1e30)
        probs = jax.nn.softmax(scores, axis=-1).astype(jnp.bfloat16).astype(jnp.float32)
        mixed = jnp.einsum('grqk,kgd->qrgd', probs, values)
        return mixed.astype(jnp.bfloat16).reshape(TOKENS_DEV, q_width)

    def layer_step(state, params):
        g_attn, query_w, out_w, g_mlp, gate_w, up_w, down_w = params
        u_attn = rms_norm(state, g_attn)
        query = jnp.dot(u_attn, query_w.reshape(D_MODEL, q_width), preferred_element_type=jnp.float32).astype(jnp.bfloat16)
        query = query.reshape(SHARDS, TOKENS_DEV, Q_PER_KV, KV_HEADS, HEAD_DIM).astype(jnp.float32)
        attended = lax.map(block_attention, (query, blk_pos, blk_seg)).reshape(SEQ_LEN, q_width)
        attn_out = jnp.dot(attended, out_w.reshape(q_width, D_MODEL), preferred_element_type=jnp.float32).astype(jnp.bfloat16)
        state = state + attn_out
        u_mlp = rms_norm(state, g_mlp)
        gate_val = jnp.dot(u_mlp, gate_w, preferred_element_type=jnp.float32).astype(jnp.bfloat16)
        up_val = jnp.dot(u_mlp, up_w, preferred_element_type=jnp.float32).astype(jnp.bfloat16)
        act_val = (jax.nn.silu(gate_val.astype(jnp.float32)) * up_val.astype(jnp.float32)).astype(jnp.bfloat16)
        down_val = jnp.dot(act_val, down_w, preferred_element_type=jnp.float32).astype(jnp.bfloat16)
        return state + down_val, None

    result, _ = lax.scan(layer_step, hidden, (norm_attn, w_query, w_out, norm_mlp, w_gate, w_up, w_down))
    return result
```

```python
import functools
import jax
import jax.numpy as jnp
from jax import lax
from jax.experimental import pallas as pl
from jax.experimental.pallas import tpu as pltpu
from jax.sharding import PartitionSpec as P

NORM_EPS = 1e-6
MESH = pl.DeviceIdType.MESH
LOG2E = 1.4426950408889634
BIG = 2.0 ** 127
NT = (((1,), (1,)), ((), ()))
F32 = jnp.float32
BF16 = jnp.bfloat16


def dest_of(me, n, step):
    chips = n // 2
    q = step // 2
    half = chips // 2
    d_chip = jnp.where(q == 0, half, jnp.where(q == 1, 1, jnp.where(q == chips - 1, 0, chips - 1)))
    d_core = jnp.where(q == chips - 1, 1 - lax.rem(step, 2), lax.rem(step, 2))
    chip = lax.rem(me // 2 + d_chip, chips)
    core = lax.rem(lax.rem(me, 2) + d_core, 2)
    return chip * 2 + core


def attn_kernel(n, heads, hd, hid_ref, seg_ref, gkv_ref, gq_ref, wk_hbm, wq_hbm, wv_hbm, o_ref,
                ukv, uq, wbuf, ks, qs, vs, kr, qr, vr, segr, fk, fq, osend, orecv,
                wsem, ssem, rsem, seg_ss, seg_rs, o_ss, o_rs):
    me = lax.axis_index('sp')
    tokens, d_model = hid_ref.shape
    hw = heads * hd
    pw = 2 * hd
    groups = heads // 2

    def wcopy(step, slot):
        d = dest_of(me, n, step)
        rows = pl.ds(pl.multiple_of(d * hw, hw), hw)
        return [pltpu.make_async_copy(w.at[rows, :], wbuf.at[slot, i], wsem.at[slot, i])
                for i, w in enumerate((wk_hbm, wq_hbm, wv_hbm))]

    for slot in range(2):
        for c in wcopy(slot, slot):
            c.start()

    barrier = pltpu.get_barrier_semaphore()
    for off in range(1, n):
        pl.semaphore_signal(barrier, inc=1, device_id={'sp': lax.rem(me + off, n)}, device_id_type=MESH)

    x = hid_ref[...].astype(F32)
    inv = lax.rsqrt(jnp.mean(x * x, axis=-1, keepdims=True) + NORM_EPS)
    xn = x * inv
    ukv[...] = (xn * gkv_ref[...].astype(F32)).astype(BF16)
    uq[...] = (xn * gq_ref[...].astype(F32)).astype(BF16)
    segr[me] = seg_ref[...]

    pl.semaphore_wait(barrier, n - 1)

    def seg_copy(p):
        return pltpu.make_async_remote_copy(seg_ref, segr.at[me], seg_ss.at[p], seg_rs.at[me],
                                            device_id={'sp': p}, device_id_type=MESH)

    def qkv_copies(g, step, p):
        bufs = ((ks, kr), (qs, qr), (vs, vr))
        return [pltpu.make_async_remote_copy(s.at[g, step], r.at[g, me], ssem.at[g, i, step], rsem.at[g, i, me],
                                             device_id={'sp': p}, device_id_type=MESH)
                for i, (s, r) in enumerate(bufs)]

    def project(slot):
        k = lax.dot_general(ukv[...], wbuf[slot, 0], NT, preferred_element_type=F32).astype(BF16)
        q = lax.dot_general(wbuf[slot, 1], uq[...], NT, preferred_element_type=F32).astype(BF16)
        v = lax.dot_general(wbuf[slot, 2], ukv[...], NT, preferred_element_type=F32).astype(BF16)
        return k, q, v

    for off in range(1, n):
        seg_copy(lax.rem(me + off, n)).start()

    def proj_step(step, _):
        slot = lax.rem(step, 2)
        for c in wcopy(step, slot):
            c.wait()
        k, q, v = project(slot)
        for g in range(groups):
            ks[g, step] = k[:, g * pw:(g + 1) * pw]
            qs[g, step] = q[g * pw:(g + 1) * pw]
            vs[g, step] = v[g * pw:(g + 1) * pw]
        for c in qkv_copies(0, step, dest_of(me, n, step)):
            c.start()

        @pl.when(step + 2 < n)
        def _():
            for c in wcopy(step + 2, slot):
                c.start()
        return 0

    lax.fori_loop(0, n - 1, proj_step, 0)
    for g in range(1, groups):
        for step in range(n - 1):
            for c in qkv_copies(g, step, dest_of(me, n, step)):
                c.start()
    for c in wcopy(n - 1, (n - 1) % 2):
        c.wait()
    k, q, v = project((n - 1) % 2)
    for g in range(groups):
        kr[g, me] = k[:, g * pw:(g + 1) * pw]
        qr[g, me] = q[g * pw:(g + 1) * pw]
        vr[g, me] = v[g * pw:(g + 1) * pw]

    for off in range(1, n):
        p = lax.rem(me + off, n)
        pltpu.make_async_remote_copy(seg_ref, segr.at[p], seg_ss.at[p], seg_rs.at[p],
                                     device_id={'sp': p}, device_id_type=MESH).wait_recv()
    ids = lax.broadcasted_iota(jnp.int32, (128, tokens), 0)
    for p in range(n):
        same = ids == segr[p]
        fq[p] = jnp.where(same, 1.0, 0.0).astype(BF16)
        fk[p] = jnp.where(same, 0.0, -BIG).T.astype(BF16)

    scale = (hd ** -0.5) * LOG2E
    kpos = lax.broadcasted_iota(jnp.int32, (tokens, tokens), 0)
    qpos = lax.broadcasted_iota(jnp.int32, (tokens, tokens), 1)
    zero = jnp.zeros((hd, tokens), BF16)

    for g in range(groups):
        for off in range(1, n):
            p = lax.rem(me + off, n)
            for i, r in enumerate((kr, qr, vr)):
                pltpu.make_async_remote_copy(r.at[g, p], r.at[g, p], ssem.at[g, i, 0], rsem.at[g, i, p],
                                             device_id={'sp': p}, device_id_type=MESH).wait_recv()

        def q_step(step, _):
            j = dest_of(me, n, step)
            qa = jnp.concatenate([qr[g, j, 0:hd], zero, fq[j]], axis=0)
            qb = jnp.concatenate([zero, qr[g, j, hd:pw], fq[j]], axis=0)

            def scores(i):
                kx = jnp.concatenate([kr[g, i], fk[i]], axis=1)
                return (jnp.dot(kx, qa, preferred_element_type=F32), jnp.dot(kx, qb, preferred_element_type=F32))

            def first(s, v):
                s = jnp.where(kpos <= qpos, s, -BIG)
                m = jnp.max(s, axis=0, keepdims=True)
                p = jnp.exp2((s - m) * scale)
                l = jnp.sum(p, axis=0, keepdims=True)
                return m, l, jnp.dot(v, p.astype(BF16), preferred_element_type=F32)

            def more(s, v, m, l, acc):
                m2 = jnp.maximum(m, jnp.max(s, axis=0, keepdims=True))
                p = jnp.exp2((s - m2) * scale)
                al = jnp.exp2((m - m2) * scale)
                l = l * al + jnp.sum(p, axis=0, keepdims=True)
                return m2, l, acc * al + jnp.dot(v, p.astype(BF16), preferred_element_type=F32)

            sa, sb = scores(j)
            ca = first(sa, vr[g, j, 0:hd])
            cb = first(sb, vr[g, j, hd:pw])

            def body(i, c):
                sa, sb = scores(i)
                return more(sa, vr[g, i, 0:hd], *c[:3]) + more(sb, vr[g, i, hd:pw], *c[3:])

            ma, la, acca, mb, lb, accb = lax.fori_loop(0, j, body, ca + cb)
            ot = jnp.concatenate([acca / la, accb / lb], axis=0).T.astype(BF16)

            @pl.when(step < n - 1)
            def _():
                osend[g, step] = ot
                pltpu.make_async_remote_copy(
                    osend.at[g, step], orecv.at[:, pl.ds(pl.multiple_of(me * hw + g * pw, pw), pw)],
                    o_ss.at[g, step], o_rs.at[g, me], device_id={'sp': j}, device_id_type=MESH).start()

            @pl.when(step == n - 1)
            def _():
                orecv[:, pl.ds(pl.multiple_of(me * hw + g * pw, pw), pw)] = ot
            return 0

        lax.fori_loop(0, n, q_step, 0)

    for g in range(groups):
        for step in range(n - 1):
            p = dest_of(me, n, step)
            pltpu.make_async_remote_copy(
                osend.at[g, step], orecv.at[:, pl.ds(pl.multiple_of(p * hw + g * pw, pw), pw)],
                o_ss.at[g, step], o_rs.at[g, p], device_id={'sp': p}, device_id_type=MESH).wait_recv()
    o_ref[...] = orecv[...]
    for g in range(groups):
        for step in range(n - 1):
            p = dest_of(me, n, step)
            for c in qkv_copies(g, step, p):
                c.wait_send()
            pltpu.make_async_remote_copy(
                osend.at[g, step], orecv.at[:, pl.ds(pl.multiple_of(me * hw + g * pw, pw), pw)],
                o_ss.at[g, step], o_rs.at[g, me], device_id={'sp': p}, device_id_type=MESH).wait_send()
    for off in range(1, n):
        seg_copy(lax.rem(me + off, n)).wait_send()


def attention(n, hidden, seg_ids, g_kv, g_q, w_key, w_value, w_query):
    tokens, d_model = hidden.shape
    _, q_heads, hd = w_query.shape
    heads = q_heads // n
    hw, pw, groups = heads * hd, 2 * hd, heads // 2
    flat = lambda w: w.transpose(1, 2, 0).reshape(q_heads * hd, d_model)
    vm = pl.BlockSpec(memory_space=pltpu.VMEM)
    hbm = pl.BlockSpec(memory_space=pl.ANY)
    dma = pltpu.SemaphoreType.DMA
    kshape, tshape = (groups, n, tokens, pw), (groups, n, pw, tokens)
    return pl.pallas_call(
        functools.partial(attn_kernel, n, heads, hd),
        out_shape=jax.ShapeDtypeStruct((tokens, n * hw), BF16),
        in_specs=[vm] * 4 + [hbm] * 3,
        out_specs=vm,
        scratch_shapes=[
            pltpu.VMEM((tokens, d_model), BF16), pltpu.VMEM((tokens, d_model), BF16),
            pltpu.VMEM((2, 3, hw, d_model), BF16),
            pltpu.VMEM(kshape, BF16), pltpu.VMEM(tshape, BF16), pltpu.VMEM(tshape, BF16),
            pltpu.VMEM(kshape, BF16), pltpu.VMEM(tshape, BF16), pltpu.VMEM(tshape, BF16),
            pltpu.VMEM((n, 1, tokens), jnp.int32),
            pltpu.VMEM((n, tokens, 128), BF16), pltpu.VMEM((n, 128, tokens), BF16),
            pltpu.VMEM(kshape, BF16), pltpu.VMEM((tokens, n * hw), BF16),
            dma((2, 3)), dma((groups, 3, n)), dma((groups, 3, n)), dma((n,)), dma((n,)), dma((groups, n)), dma((groups, n)),
        ],
        compiler_params=pltpu.CompilerParams(collective_id=0, has_side_effects=True, vmem_limit_bytes=60 * 2 ** 20),
    )(hidden, seg_ids.reshape(1, tokens), g_kv.reshape(1, d_model), g_q.reshape(1, d_model),
      flat(w_key), flat(w_query), flat(w_value))


def mlp_kernel(tile, depth, o_ref, h_ref, gm_ref, wo_hbm, wg_hbm, wu_hbm, wd_hbm, out_ref,
               wo, rg, ru, rd, u, h1, acc, cbuf, so, sg, su, sd):
    tokens, d_model = h_ref.shape
    ff = wg_hbm.shape[1]
    nf = ff // tile
    no = d_model // tile

    def cols(f):
        return pl.ds(pl.multiple_of(f * tile, tile), tile)

    def cg(f):
        s = lax.rem(f, depth)
        return pltpu.make_async_copy(wg_hbm.at[:, cols(f)], rg.at[s], sg.at[s])

    def cu(f):
        s = lax.rem(f, depth)
        return pltpu.make_async_copy(wu_hbm.at[:, cols(f)], ru.at[s], su.at[s])

    def cd(f):
        s = lax.rem(f, depth)
        return pltpu.make_async_copy(wd_hbm.at[cols(f), :], rd.at[s], sd.at[s])

    co = [pltpu.make_async_copy(wo_hbm.at[:, cols(i)], wo.at[i], so.at[i]) for i in range(no)]
    for c in co:
        c.start()
    for f in range(depth):
        cg(jnp.int32(f)).start()
        cu(jnp.int32(f)).start()
        cd(jnp.int32(f)).start()

    ssq = jnp.zeros((tokens, 1), F32)
    for i in range(no):
        co[i].wait()
        a = jnp.dot(o_ref[...], wo[i], preferred_element_type=F32).astype(BF16)
        s = pl.ds(i * tile, tile)
        h = (h_ref[:, s].astype(F32) + a.astype(F32)).astype(BF16)
        h1[:, s] = h
        h = h.astype(F32)
        ssq += jnp.sum(h * h, axis=-1, keepdims=True)
    inv = lax.rsqrt(ssq / d_model + NORM_EPS)
    u[...] = (h1[...].astype(F32) * inv * gm_ref[...].astype(F32)).astype(BF16)

    def gate_up(f):
        s = lax.rem(f, depth)
        cg(f).wait()
        cu(f).wait()
        a = jnp.dot(u[...], rg[s], preferred_element_type=F32).astype(BF16).astype(F32)
        b = jnp.dot(u[...], ru[s], preferred_element_type=F32).astype(BF16).astype(F32)

        @pl.when(f + depth < nf)
        def _():
            cg(f + depth).start()
            cu(f + depth).start()
        return (jax.nn.silu(a) * b).astype(BF16)

    def down(f, c):
        s = lax.rem(f, depth)
        cd(f).wait()
        d = jnp.dot(c, rd[s], preferred_element_type=F32)

        @pl.when(f + depth < nf)
        def _():
            cd(f + depth).start()
        return d

    cbuf[0] = gate_up(jnp.int32(0))
    acc[...] = jnp.zeros_like(acc)

    def step(f, _):
        acc[...] += down(f - 1, cbuf[lax.rem(f - 1, 2)])
        cbuf[lax.rem(f, 2)] = gate_up(f)
        return 0

    lax.fori_loop(1, nf, step, 0)
    d = acc[...] + down(jnp.int32(nf - 1), cbuf[(nf - 1) % 2])
    out_ref[...] = (h1[...].astype(F32) + d.astype(BF16).astype(F32)).astype(BF16)


def mlp(o, hidden, g_mlp, w_out, w_gate, w_up, w_down):
    tokens, d_model = hidden.shape
    ff = w_gate.shape[1]
    tile, depth = 512, 4
    vm = pl.BlockSpec(memory_space=pltpu.VMEM)
    hbm = pl.BlockSpec(memory_space=pl.ANY)
    dma = pltpu.SemaphoreType.DMA
    no = d_model // tile
    return pl.pallas_call(
        functools.partial(mlp_kernel, tile, depth),
        out_shape=jax.ShapeDtypeStruct((tokens, d_model), BF16),
        in_specs=[vm] * 3 + [hbm] * 4,
        out_specs=vm,
        scratch_shapes=[
            pltpu.VMEM((no, d_model, tile), BF16),
            pltpu.VMEM((depth, d_model, tile), BF16), pltpu.VMEM((depth, d_model, tile), BF16),
            pltpu.VMEM((depth, tile, d_model), BF16),
            pltpu.VMEM((tokens, d_model), BF16), pltpu.VMEM((tokens, d_model), BF16),
            pltpu.VMEM((tokens, d_model), F32), pltpu.VMEM((2, tokens, tile), BF16),
            dma((no,)), dma((depth,)), dma((depth,)), dma((depth,)),
        ],
        compiler_params=pltpu.CompilerParams(vmem_limit_bytes=60 * 2 ** 20),
    )(o, hidden, g_mlp.reshape(1, d_model), w_out.reshape(-1, d_model), w_gate, w_up, w_down)


def solution(mesh):
    n = mesh.shape['sp']

    def body(hidden, seg_ids, norm_kv, w_key, w_value, norm_attn, w_query, w_out, norm_mlp, w_gate, w_up, w_down):
        o = attention(n, hidden, seg_ids, norm_kv, norm_attn[0], w_key, w_value, w_query[0])
        return mlp(o, hidden, norm_mlp[0], w_out[0], w_gate[0], w_up[0], w_down[0])

    row_spec = P(('dp', 'sp'), None)
    in_specs = (row_spec, P(('dp', 'sp'))) + (P(),) * 10
    return jax.shard_map(body, mesh=mesh, in_specs=in_specs, out_specs=row_spec, check_vma=False)
```

```python
import functools
import jax
import jax.numpy as jnp
from jax import lax
from jax.experimental import pallas as pl
from jax.experimental.pallas import tpu as pltpu
from jax.sharding import PartitionSpec as P

NORM_EPS = 1e-6
MESH = pl.DeviceIdType.MESH
LOG2E = 1.4426950408889634
BIG = 2.0 ** 127
NT = (((1,), (1,)), ((), ()))
F32 = jnp.float32
BF16 = jnp.bfloat16


def dest_of(me, n, step):
    chips = n // 2
    q = step // 2
    half = chips // 2
    d_chip = jnp.where(q == 0, half, jnp.where(q == 1, 1, jnp.where(q == chips - 1, 0, chips - 1)))
    d_core = jnp.where(q == chips - 1, 1 - lax.rem(step, 2), lax.rem(step, 2))
    chip = lax.rem(me // 2 + d_chip, chips)
    core = lax.rem(lax.rem(me, 2) + d_core, 2)
    return chip * 2 + core


def kernel(n, heads, hd, tile, nr, hid_ref, seg_ref, gkv_ref, gq_ref, gm_ref, wk_hbm, wq_hbm, wv_hbm,
           wo_hbm, wg_hbm, wu_hbm, wd_hbm, out_ref,
           ukv, uq, ring, ks, qs, vs, kr, qr, vr, segr, fk, fq, osend, orecv, s_scr, p_scr, ab, c_ref,
           wsem, sr, ssem, rsem, seg_ss, seg_rs, o_ss, o_rs):
    me = lax.axis_index('sp')
    tokens, d_model = hid_ref.shape
    ff = wg_hbm.shape[1]
    hw = heads * hd
    pw = 2 * hd
    groups = heads // 2
    nf = ff // tile
    no = d_model // tile

    def remote(s, d, ss, rs, p):
        return pltpu.make_async_remote_copy(s, d, ss, rs, device_id={'sp': p}, device_id_type=MESH)

    kp = d_model // tile
    nc = ff // d_model

    def wpieces(slot, i):
        b = slot * 3 + i
        per = tile // hw
        row = lax.rem(b, per) * kp * hw
        return [ring.at[nr - 5 + b // per, pl.ds(pl.multiple_of(row + k * hw, hw), hw)] for k in range(kp)]

    def wcopy(step):
        slot = lax.rem(step, 3)
        d = dest_of(me, n, step)
        rows = pl.ds(pl.multiple_of(d * hw, hw), hw)
        return [pltpu.make_async_copy(w.at[rows, k * tile:(k + 1) * tile], dst, wsem.at[slot, i, k])
                for i, w in enumerate((wk_hbm, wq_hbm, wv_hbm)) for k, dst in enumerate(wpieces(slot, i))]

    def cols(f):
        return pl.ds(pl.multiple_of(f * tile, tile), tile)

    def chunk(w, c, src):
        s = lax.rem(c, nr)
        return pltpu.make_async_copy(src, ring.at[s], sr.at[s])

    def out_copy(i):
        return chunk(wo_hbm, i, wo_hbm.at[:, cols(i)])

    def gate_copy(f):
        return chunk(wg_hbm, no + 2 * f, wg_hbm.at[:, cols(f)])

    def up_copy(f):
        return chunk(wu_hbm, no + 2 * f + 1, wu_hbm.at[:, cols(f)])

    def down_copy(m):
        rows = pl.ds(pl.multiple_of(lax.rem(m, nc) * d_model, d_model), d_model)
        return chunk(wd_hbm, no + 2 * nf + m, wd_hbm.at[rows, cols(m // nc)])

    def refill_gu(f):
        @pl.when(f < nf)
        def _():
            gate_copy(f).start()
            up_copy(f).start()

        @pl.when(f >= nf)
        def _():
            down_copy(2 * (f - nf)).start()
            down_copy(2 * (f - nf) + 1).start()

    for step in range(2):
        for c in wcopy(jnp.int32(step)):
            c.start()

    barrier = pltpu.get_barrier_semaphore()
    for off in range(1, n):
        pl.semaphore_signal(barrier, inc=1, device_id={'sp': lax.rem(me + off, n)}, device_id_type=MESH)

    def gain(ref):
        return jnp.concatenate([ref[i:i + 1].astype(F32) for i in range(d_model // 128)], axis=1)

    x = hid_ref[...].astype(F32)
    xn = x * lax.rsqrt(jnp.mean(x * x, axis=-1, keepdims=True) + NORM_EPS)
    ukv[...] = (xn * gain(gkv_ref)).astype(BF16)
    uq[...] = (xn * gq_ref[...].astype(F32)).astype(BF16)
    segr[me] = seg_ref[...]

    def seg_copy(p):
        return remote(seg_ref, segr.at[me], seg_ss.at[p], seg_rs.at[me], p)

    def qkv_copies(g, step, p):
        bufs = ((ks, kr), (qs, qr), (vs, vr))
        return [remote(s.at[g, step], r.at[g, me], ssem.at[g, i, step], rsem.at[g, i, me], p)
                for i, (s, r) in enumerate(bufs)]

    def project(step):
        for c in wcopy(step):
            c.wait()

        @pl.when(step + 2 < n)
        def _():
            for c in wcopy(step + 2):
                c.start()
        slot = lax.rem(step, 3)

        u_kv = [ukv[:, i * tile:(i + 1) * tile] for i in range(kp)]
        u_q = [uq[:, i * tile:(i + 1) * tile] for i in range(kp)]
        w = [[p[...] for p in wpieces(slot, i)] for i in range(3)]

        def nt(a, b):
            return sum(lax.dot_general(x, y, NT, preferred_element_type=F32) for x, y in zip(a, b)).astype(BF16)

        k, q, v = nt(u_kv, w[0]), nt(w[1], u_q), nt(w[2], u_kv)
        return k, q, v

    def store(step):
        k, q, v = project(step)
        for g in range(groups):
            ks[g, step] = k[:, g * pw:(g + 1) * pw]
            qs[g, step] = q[g * pw:(g + 1) * pw]
            vs[g, step] = v[g * pw:(g + 1) * pw]

    def send(g, step):
        for c in qkv_copies(g, step, dest_of(me, n, step)):
            c.start()

    def proj_step(step, _):
        store(step)

        @pl.when(step == lead_steps - 1)
        def _():
            pl.semaphore_wait(barrier, n - 1)
            for s in range(lead_steps - 1):
                send(0, s)
            for off in range(1, n):
                seg_copy(lax.rem(me + off, n)).start()

        @pl.when(step >= lead_steps - 1)
        def _():
            send(0, step)
        return 0

    lead_steps = 2
    lax.fori_loop(0, n - 1, proj_step, 0)
    for g in range(1, groups):
        for step in range(n - 1):
            send(g, step)
    lead = nr - 5
    for i in range(no):
        out_copy(i).start()
    for f in range((lead - no + 1) // 2):
        gate_copy(f).start()
        if no + 2 * f + 1 < lead:
            up_copy(f).start()
    k, q, v = project(jnp.int32(n - 1))
    for g in range(groups):
        kr[g, me] = k[:, g * pw:(g + 1) * pw]
        qr[g, me] = q[g * pw:(g + 1) * pw]
        vr[g, me] = v[g * pw:(g + 1) * pw]
    for c in range(lead, nr):
        (up_copy if (c - no) % 2 else gate_copy)((c - no) // 2).start()

    for off in range(1, n):
        p = lax.rem(me + off, n)
        remote(seg_ref, segr.at[p], seg_ss.at[p], seg_rs.at[p], p).wait_recv()
    ids = lax.broadcasted_iota(jnp.int32, (128, tokens), 0)

    def features(p, _):
        same = ids == segr[p]
        fq[p] = jnp.where(same, 1.0, 0.0).astype(BF16)
        fk[p] = jnp.where(same, 0.0, -BIG).T.astype(BF16)
        return 0

    lax.fori_loop(0, n, features, 0)

    scale = (hd ** -0.5) * LOG2E
    kpos = lax.broadcasted_iota(jnp.int32, (tokens, tokens), 0)
    qpos = lax.broadcasted_iota(jnp.int32, (tokens, tokens), 1)
    zero = jnp.zeros((hd, tokens), BF16)
    ones = jnp.ones((16, tokens), BF16)
    half = n // 2
    low = jnp.minimum(me, n - 1 - me)

    def o_cols(d, g):
        return orecv.at[:, pl.ds(pl.multiple_of(d * hw + g * pw, pw), pw)]

    def o_copy(g, j):
        return remote(osend.at[g, j], o_cols(me, g), o_ss.at[g, j], o_rs.at[g, me], j)

    def attend(g, j1):
        j2 = n - 1 - j1

        def q_ext(j):
            return (jnp.concatenate([qr[g, j, 0:hd], zero, fq[j]], axis=0),
                    jnp.concatenate([zero, qr[g, j, hd:pw], fq[j]], axis=0))

        qa, qb = q_ext(j1), q_ext(j2)

        def block(t):
            if t < 2:
                return (j1, j2)[t], t == 0
            first = t - 2 < j1
            return jnp.where(first, j1 + 1 - t, n - t), first

        def scores(t):
            i, first = block(t)
            kx = jnp.concatenate([kr[g, i], fk[i]], axis=1)
            for h in range(2):
                if t < 2:
                    q = (qa, qb)[t][h]
                else:
                    q = qb[h] if t > half else jnp.where(first, qa[h], qb[h])
                s_scr[t % 2, h] = jnp.dot(kx, q, preferred_element_type=F32)

        m_a, m_b, m = [None] * 2, [None] * 2, [None] * 2
        acc_a, acc_b, acc = [None] * 2, [None] * 2, [None] * 2
        alpha = {}

        def soft(t):
            for h in range(2):
                s = s_scr[t % 2, h]
                if t < 2:
                    s = jnp.where(kpos <= qpos, s, -BIG)
                    new = jnp.max(s, axis=0, keepdims=True)
                    (m_a, m_b)[t][h] = new
                else:
                    old = m_a[h] if t == 2 else m[h]
                    if t - 2 < half:
                        old = jnp.where(t - 2 == j1, m_b[h], old)
                    new = jnp.maximum(old, jnp.max(s, axis=0, keepdims=True))
                    alpha[t, h] = jnp.exp2((old - new) * scale)
                    m[h] = new
                p_scr[t % 2, h] = jnp.exp2((s - new) * scale).astype(BF16)

        def mix(t):
            i, _ = block(t)
            for h in range(2):
                vx = jnp.concatenate([vr[g, i, h * hd:(h + 1) * hd], ones], axis=0)
                d = jnp.dot(vx, p_scr[t % 2, h], preferred_element_type=F32)
                if t == 0:
                    acc[h] = d
                elif t == 1:
                    acc_b[h] = d
                else:
                    if t - 2 < half:
                        swap = t - 2 == j1
                        acc_a[h] = acc[h] if t == 2 else jnp.where(swap, acc[h], acc_a[h])
                        acc[h] = jnp.where(swap, acc_b[h], acc[h])
                    acc[h] = acc[h] * alpha[t, h] + d

        scores(0)
        for t in range(n + 2):
            if t < n:
                scores(t + 1)
            if t < n + 1:
                soft(t)
            if t >= 1:
                mix(t - 1)
        return [jnp.concatenate([r[h][0:hd] / r[h][hd:hd + 1] for h in range(2)], axis=0).T.astype(BF16)
                for r in (acc_a, acc)]

    def group(g, _):
        for off in range(1, n):
            p = lax.rem(me + off, n)
            for i, r in enumerate((kr, qr, vr)):
                remote(r.at[g, p], r.at[g, p], ssem.at[g, i, 0], rsem.at[g, i, p], p).wait_recv()

        def unit(t, _):
            j1 = lax.rem(low + 1 + t, half)
            for j, o in zip((j1, n - 1 - j1), attend(g, j1)):
                osend[g, j] = o

                @pl.when(j != me)
                def _():
                    o_copy(g, j).start()
            return 0

        lax.fori_loop(0, half, unit, 0)
        orecv[:, pl.ds(pl.multiple_of(me * hw + g * pw, pw), pw)] = osend[g, me]
        return 0

    lax.fori_loop(0, groups, group, 0)

    for g in range(groups):
        for off in range(1, n):
            p = lax.rem(me + off, n)
            remote(osend.at[g, p], o_cols(p, g), o_ss.at[g, p], o_rs.at[g, p], p).wait_recv()

    h1, u = uq, ukv
    ssq = jnp.zeros((tokens, 1), F32)
    for i in range(no):
        out_copy(i).wait()
        a = jnp.dot(orecv[...], ring[i], preferred_element_type=F32).astype(BF16)
        s = pl.ds(i * tile, tile)
        h = (hid_ref[:, s].astype(F32) + a.astype(F32)).astype(BF16)
        h1[:, s] = h
        h = h.astype(F32)
        ssq += jnp.sum(h * h, axis=-1, keepdims=True)
    for i in range(no // 2):
        refill_gu(jnp.int32((nr - no) // 2 + i))
    inv = lax.rsqrt(ssq / d_model + NORM_EPS)
    u[...] = (h1[...].astype(F32) * inv * gm_ref[...].astype(F32)).astype(BF16)

    def gate_up(f):
        gate_copy(f).wait()
        up_copy(f).wait()
        s = lax.rem(no + 2 * f, nr)
        return [jnp.dot(u[...], ring[s + i], preferred_element_type=F32).astype(BF16) for i in range(2)]

    def act(f):
        a = ab[0].astype(F32)
        c_ref[:, cols(f)] = (jax.nn.silu(a) * ab[1].astype(F32)).astype(BF16)

    ab[0], ab[1] = gate_up(jnp.int32(0))
    refill_gu(jnp.int32(nr // 2))

    def mlp_step(f, _):
        a, b = gate_up(f)
        act(f - 1)
        ab[0] = a
        ab[1] = b

        @pl.when(f + nr // 2 < nf + no * nc // 2)
        def _():
            refill_gu(f + nr // 2)
        return 0

    lax.fori_loop(1, nf, mlp_step, 0)
    act(jnp.int32(nf - 1))

    def down_step(j, _):
        d = None
        for i in range(nc):
            m = j * nc + i
            down_copy(m).wait()
            part = jnp.dot(c_ref[:, i * d_model:(i + 1) * d_model], ring[lax.rem(no + 2 * nf + m, nr)],
                           preferred_element_type=F32)
            d = part if d is None else d + part
        out_ref[:, cols(j)] = (h1[:, cols(j)].astype(F32) + d.astype(BF16).astype(F32)).astype(BF16)
        return 0

    lax.fori_loop(0, no, down_step, 0)

    for g in range(groups):
        for step in range(n - 1):
            for c in qkv_copies(g, step, dest_of(me, n, step)):
                c.wait_send()
        for off in range(1, n):
            o_copy(g, lax.rem(me + off, n)).wait_send()
    for off in range(1, n):
        seg_copy(lax.rem(me + off, n)).wait_send()


def decoder(n, hidden, seg_ids, g_kv, g_q, g_mlp, w_key, w_value, w_query, w_out, w_gate, w_up, w_down):
    tokens, d_model = hidden.shape
    _, q_heads, hd = w_query.shape
    heads = q_heads // n
    hw, pw, groups = heads * hd, 2 * hd, heads // 2
    tile, nr = 512, 18
    flat = lambda w: w.transpose(1, 2, 0).reshape(q_heads * hd, d_model)
    row = lambda g: g.reshape(1, d_model)
    vm = pl.BlockSpec(memory_space=pltpu.VMEM)
    hbm = pl.BlockSpec(memory_space=pl.ANY)
    dma = pltpu.SemaphoreType.DMA
    vb = lambda *s: pltpu.VMEM(s, BF16)
    kshape, tshape = (groups, n, tokens, pw), (groups, n, pw, tokens)
    return pl.pallas_call(
        functools.partial(kernel, n, heads, hd, tile, nr),
        out_shape=jax.ShapeDtypeStruct((tokens, d_model), BF16),
        in_specs=[vm] * 5 + [hbm] * 7,
        out_specs=vm,
        scratch_shapes=[
            vb(tokens, d_model), vb(tokens, d_model), vb(nr, d_model, tile),
            vb(*kshape), vb(*tshape), vb(*tshape), vb(*kshape), vb(*tshape), vb(*tshape),
            pltpu.VMEM((n, 1, tokens), jnp.int32), vb(n, tokens, 128), vb(n, 128, tokens),
            vb(*kshape), vb(tokens, n * hw),
            pltpu.VMEM((2, 2, tokens, tokens), F32), vb(2, 2, tokens, tokens),
            vb(2, tokens, tile), vb(tokens, w_gate.shape[1]),
            dma((3, 3, d_model // tile)), dma((nr,)), dma((groups, 3, n)), dma((groups, 3, n)), dma((n,)), dma((n,)),
            dma((groups, n)), dma((groups, n)),
        ],
        compiler_params=pltpu.CompilerParams(collective_id=0, has_side_effects=True, vmem_limit_bytes=67043328),
    )(hidden, seg_ids.reshape(1, tokens), g_kv.reshape(d_model // 128, 128), row(g_q), row(g_mlp), flat(w_key), flat(w_query), flat(w_value),
      w_out.reshape(-1, d_model), w_gate, w_up, w_down)


def solution(mesh):
    n = mesh.shape['sp']

    def body(hidden, seg_ids, norm_kv, w_key, w_value, norm_attn, w_query, w_out, norm_mlp, w_gate, w_up, w_down):
        return decoder(n, hidden, seg_ids, norm_kv, norm_attn[0], norm_mlp[0], w_key, w_value, w_query[0], w_out[0],
                       w_gate[0], w_up[0], w_down[0])

    row_spec = P(('dp', 'sp'), None)
    in_specs = (row_spec, P(('dp', 'sp'))) + (P(),) * 10
    return jax.shard_map(body, mesh=mesh, in_specs=in_specs, out_specs=row_spec, check_vma=False)
```

```python
import functools
import jax
import jax.numpy as jnp
from jax import lax
from jax.experimental import pallas as pl
from jax.experimental.pallas import tpu as pltpu
from jax.sharding import PartitionSpec as P

NORM_EPS = 1e-6
MESH = pl.DeviceIdType.MESH
LOG2E = 1.4426950408889634
BIG = 2.0 ** 127
NT = (((1,), (1,)), ((), ()))
F32 = jnp.float32
BF16 = jnp.bfloat16


def route(me, n):
    chips = n // 2
    assert chips == 4
    chip, core = me // 2, lax.rem(me, 2)
    turn = 1 - 2 * core
    ahead = lax.rem(chip + turn + chips, chips) * 2
    behind = lax.rem(chip - turn + chips, chips) * 2
    return ahead, behind, chip * 2 + 1 - core, behind + core


def dest_of(me, n, step):
    ahead, behind, other, _ = route(me, n)
    pair = jnp.where(step < 4, behind, ahead) + lax.rem(step, 4)
    return jnp.where(lax.rem(step, 4) < 2, pair, jnp.where(lax.rem(step, 4) == 2, other, me))


def kernel(n, heads, hd, tile, nr, hid_ref, seg_ref, gkv_ref, gq_ref, gm_ref, wk_hbm, wq_hbm, wv_hbm,
           wo_hbm, wg_hbm, wu_hbm, wd_hbm, out_ref,
           ukv, uq, ring, ks, qs, vs, kr, qr, vr, segr, fk, fq, osend, orecv, s_scr, p_scr, ab, c_ref,
           wsem, sr, hand_ss, hand_rs, ssem, rsem, seg_ss, seg_rs, o_ss, o_rs):
    me = lax.axis_index('sp')
    tokens, d_model = hid_ref.shape
    ff = wg_hbm.shape[1]
    hw = heads * hd
    pw = 2 * hd
    groups = heads // 2
    nf = ff // tile
    no = d_model // tile

    def remote(s, d, ss, rs, p):
        return pltpu.make_async_remote_copy(s, d, ss, rs, device_id={'sp': p}, device_id_type=MESH)

    kp = d_model // tile
    nc = ff // d_model

    def wpieces(slot, i):
        b = slot * 3 + i
        per = tile // hw
        row = lax.rem(b, per) * kp * hw
        return [ring.at[nr - 5 + b // per, pl.ds(pl.multiple_of(row + k * hw, hw), hw)] for k in range(kp)]

    def wcopy(step):
        slot = lax.rem(step, 3)
        d = dest_of(me, n, step)
        rows = pl.ds(pl.multiple_of(d * hw, hw), hw)
        return [pltpu.make_async_copy(w.at[rows, k * tile:(k + 1) * tile], dst, wsem.at[slot, i, k])
                for i, w in enumerate((wk_hbm, wq_hbm, wv_hbm)) for k, dst in enumerate(wpieces(slot, i))]

    def cols(f):
        return pl.ds(pl.multiple_of(f * tile, tile), tile)

    def chunk(w, c, src):
        s = lax.rem(c, nr)
        return pltpu.make_async_copy(src, ring.at[s], sr.at[s])

    def out_copy(i):
        return chunk(wo_hbm, i, wo_hbm.at[:, cols(i)])

    def gate_copy(f):
        return chunk(wg_hbm, no + 2 * f, wg_hbm.at[:, cols(f)])

    def up_copy(f):
        return chunk(wu_hbm, no + 2 * f + 1, wu_hbm.at[:, cols(f)])

    def down_copy(m):
        rows = pl.ds(pl.multiple_of(lax.rem(m, nc) * d_model, d_model), d_model)
        return chunk(wd_hbm, no + 2 * nf + m, wd_hbm.at[rows, cols(m // nc)])

    def refill_gu(f):
        @pl.when(f < nf)
        def _():
            gate_copy(f).start()
            up_copy(f).start()

        @pl.when(f >= nf)
        def _():
            down_copy(2 * (f - nf)).start()
            down_copy(2 * (f - nf) + 1).start()

    for step in range(2):
        for c in wcopy(jnp.int32(step)):
            c.start()

    barrier = pltpu.get_barrier_semaphore()
    for off in range(1, n):
        pl.semaphore_signal(barrier, inc=1, device_id={'sp': lax.rem(me + off, n)}, device_id_type=MESH)

    def gain(ref):
        return jnp.concatenate([ref[i:i + 1].astype(F32) for i in range(d_model // 128)], axis=1)

    x = hid_ref[...].astype(F32)

    def normed(x):
        xn = x * lax.rsqrt(jnp.mean(x * x, axis=-1, keepdims=True) + NORM_EPS)
        return (xn * gain(gkv_ref)).astype(BF16), (xn * gq_ref[...].astype(F32)).astype(BF16)

    ukv[...], uq[...] = normed(x)
    segr[me] = seg_ref[...]

    def seg_copy(p):
        return remote(seg_ref, segr.at[me], seg_ss.at[p], seg_rs.at[me], p)

    ahead, _, _, origin = route(me, n)
    handed = c_ref.at[:, 0:d_model]
    y_kv = c_ref.at[:, d_model:2 * d_model]
    y_q = c_ref.at[:, 2 * d_model:3 * d_model]
    hand = remote(hid_ref, handed, hand_ss, hand_rs, ahead + lax.rem(me, 2))

    def qkv_copies(g, step):
        slot = step - step // 4
        shard = jnp.where(step < 4, me, origin)
        bufs = ((ks, kr), (qs, qr), (vs, vr))
        return [remote(s.at[g, slot], r.at[g, shard], ssem.at[g, i, slot], rsem.at[g, i, shard], dest_of(me, n, step))
                for i, (s, r) in enumerate(bufs)]

    def project(step, xkv, xq):
        for c in wcopy(step):
            c.wait()

        @pl.when(step + 2 < n)
        def _():
            for c in wcopy(step + 2):
                c.start()
        slot = lax.rem(step, 3)

        u_kv = [xkv[:, i * tile:(i + 1) * tile] for i in range(kp)]
        u_q = [xq[:, i * tile:(i + 1) * tile] for i in range(kp)]
        w = [[p[...] for p in wpieces(slot, i)] for i in range(3)]

        def nt(a, b):
            return sum(lax.dot_general(x, y, NT, preferred_element_type=F32) for x, y in zip(a, b)).astype(BF16)

        k, q, v = nt(u_kv, w[0]), nt(w[1], u_q), nt(w[2], u_kv)
        return k, q, v

    def store(step, xkv, xq):
        slot = step - step // 4
        k, q, v = project(step, xkv, xq)
        for g in range(groups):
            ks[g, slot] = k[:, g * pw:(g + 1) * pw]
            qs[g, slot] = q[g * pw:(g + 1) * pw]
            vs[g, slot] = v[g * pw:(g + 1) * pw]

    def keep(step, shard, xkv, xq):
        k, q, v = project(step, xkv, xq)
        for g in range(groups):
            kr[g, shard] = k[:, g * pw:(g + 1) * pw]
            qr[g, shard] = q[g * pw:(g + 1) * pw]
            vr[g, shard] = v[g * pw:(g + 1) * pw]

    def send(g, step):
        for c in qkv_copies(g, step):
            c.start()

    def own_step(step, _):
        store(step, ukv, uq)

        @pl.when(step == 1)
        def _():
            pl.semaphore_wait(barrier, n - 1)
            hand.start()
            for off in range(1, n):
                seg_copy(lax.rem(me + off, n)).start()
        return 0

    lax.fori_loop(0, 3, own_step, 0)
    for g in range(groups):
        send(g, 2)
    keep(jnp.int32(3), me, ukv, uq)
    lead = nr - 5
    for i in range(no):
        out_copy(i).start()
    for f in range((lead - no + 1) // 2):
        gate_copy(f).start()
        if no + 2 * f + 1 < lead:
            up_copy(f).start()
    hand.wait_send()
    for g in range(groups):
        for step in range(2):
            send(g, step)
    hand.wait_recv()
    y_kv[...], y_q[...] = normed(handed[...].astype(F32))

    def handed_step(step, _):
        store(step, y_kv, y_q)
        send(0, step)
        return 0

    lax.fori_loop(4, 6, handed_step, 0)
    for g in range(1, groups):
        for step in (4, 5):
            send(g, step)
    lax.fori_loop(6, 7, handed_step, 0)
    for g in range(1, groups):
        send(g, 6)
    keep(jnp.int32(7), origin, y_kv, y_q)
    for c in range(lead, nr):
        (up_copy if (c - no) % 2 else gate_copy)((c - no) // 2).start()

    for off in range(1, n):
        p = lax.rem(me + off, n)
        remote(seg_ref, segr.at[p], seg_ss.at[p], seg_rs.at[p], p).wait_recv()
    ids = lax.broadcasted_iota(jnp.int32, (128, tokens), 0)

    def features(p, _):
        same = ids == segr[p]
        fq[p] = jnp.where(same, 1.0, 0.0).astype(BF16)
        fk[p] = jnp.where(same, 0.0, -BIG).T.astype(BF16)
        return 0

    lax.fori_loop(0, n, features, 0)

    scale = (hd ** -0.5) * LOG2E
    kpos = lax.broadcasted_iota(jnp.int32, (tokens, tokens), 0)
    qpos = lax.broadcasted_iota(jnp.int32, (tokens, tokens), 1)
    zero = jnp.zeros((hd, tokens), BF16)
    ones = jnp.ones((16, tokens), BF16)
    half = n // 2
    low = jnp.minimum(me, n - 1 - me)

    def o_cols(d, g):
        return orecv.at[:, pl.ds(pl.multiple_of(d * hw + g * pw, pw), pw)]

    def o_copy(g, j):
        return remote(osend.at[g, j], o_cols(me, g), o_ss.at[g, j], o_rs.at[g, me], j)

    def attend(g, j1):
        j2 = n - 1 - j1

        def q_ext(j):
            return (jnp.concatenate([qr[g, j, 0:hd], zero, fq[j]], axis=0),
                    jnp.concatenate([zero, qr[g, j, hd:pw], fq[j]], axis=0))

        qa, qb = q_ext(j1), q_ext(j2)

        def block(t):
            if t < 2:
                return (j1, j2)[t], t == 0
            first = t - 2 < j1
            return jnp.where(first, j1 + 1 - t, n - t), first

        def scores(t):
            i, first = block(t)
            kx = jnp.concatenate([kr[g, i], fk[i]], axis=1)
            for h in range(2):
                if t < 2:
                    q = (qa, qb)[t][h]
                else:
                    q = qb[h] if t > half else jnp.where(first, qa[h], qb[h])
                s_scr[t % 2, h] = jnp.dot(kx, q, preferred_element_type=F32)

        m_a, m_b, m = [None] * 2, [None] * 2, [None] * 2
        acc_a, acc_b, acc = [None] * 2, [None] * 2, [None] * 2
        alpha = {}

        def soft(t):
            for h in range(2):
                s = s_scr[t % 2, h]
                if t < 2:
                    s = jnp.where(kpos <= qpos, s, -BIG)
                    new = jnp.max(s, axis=0, keepdims=True)
                    (m_a, m_b)[t][h] = new
                else:
                    old = m_a[h] if t == 2 else m[h]
                    if t - 2 < half:
                        old = jnp.where(t - 2 == j1, m_b[h], old)
                    new = jnp.maximum(old, jnp.max(s, axis=0, keepdims=True))
                    alpha[t, h] = jnp.exp2((old - new) * scale)
                    m[h] = new
                p_scr[t % 2, h] = jnp.exp2((s - new) * scale).astype(BF16)

        def mix(t):
            i, _ = block(t)
            for h in range(2):
                vx = jnp.concatenate([vr[g, i, h * hd:(h + 1) * hd], ones], axis=0)
                d = jnp.dot(vx, p_scr[t % 2, h], preferred_element_type=F32)
                if t == 0:
                    acc[h] = d
                elif t == 1:
                    acc_b[h] = d
                else:
                    if t - 2 < half:
                        swap = t - 2 == j1
                        acc_a[h] = acc[h] if t == 2 else jnp.where(swap, acc[h], acc_a[h])
                        acc[h] = jnp.where(swap, acc_b[h], acc[h])
                    acc[h] = acc[h] * alpha[t, h] + d

        scores(0)
        for t in range(n + 2):
            if t < n:
                scores(t + 1)
            if t < n + 1:
                soft(t)
            if t >= 1:
                mix(t - 1)
        return [jnp.concatenate([r[h][0:hd] / r[h][hd:hd + 1] for h in range(2)], axis=0).T.astype(BF16)
                for r in (acc_a, acc)]

    def group(g, _):
        for off in range(1, n):
            p = lax.rem(me + off, n)

            @pl.when(p != origin)
            def _():
                for i, r in enumerate((kr, qr, vr)):
                    remote(r.at[g, p], r.at[g, p], ssem.at[g, i, 0], rsem.at[g, i, p], p).wait_recv()

        def unit(t, _):
            j1 = lax.rem(low + 1 + t, half)
            for j, o in zip((j1, n - 1 - j1), attend(g, j1)):
                osend[g, j] = o

                @pl.when(j != me)
                def _():
                    o_copy(g, j).start()
            return 0

        lax.fori_loop(0, half, unit, 0)
        orecv[:, pl.ds(pl.multiple_of(me * hw + g * pw, pw), pw)] = osend[g, me]
        return 0

    lax.fori_loop(0, groups, group, 0)

    for g in range(groups):
        for off in range(1, n):
            p = lax.rem(me + off, n)
            remote(osend.at[g, p], o_cols(p, g), o_ss.at[g, p], o_rs.at[g, p], p).wait_recv()

    h1, u = uq, ukv
    ssq = jnp.zeros((tokens, 1), F32)
    for i in range(no):
        out_copy(i).wait()
        a = jnp.dot(orecv[...], ring[i], preferred_element_type=F32).astype(BF16)
        s = pl.ds(i * tile, tile)
        h = (hid_ref[:, s].astype(F32) + a.astype(F32)).astype(BF16)
        h1[:, s] = h
        h = h.astype(F32)
        ssq += jnp.sum(h * h, axis=-1, keepdims=True)
    for i in range(no // 2):
        refill_gu(jnp.int32((nr - no) // 2 + i))
    inv = lax.rsqrt(ssq / d_model + NORM_EPS)
    u[...] = (h1[...].astype(F32) * inv * gm_ref[...].astype(F32)).astype(BF16)

    def gate_up(f):
        gate_copy(f).wait()
        up_copy(f).wait()
        s = lax.rem(no + 2 * f, nr)
        return [jnp.dot(u[...], ring[s + i], preferred_element_type=F32).astype(BF16) for i in range(2)]

    def act(f):
        a = ab[0].astype(F32)
        c_ref[:, cols(f)] = (jax.nn.silu(a) * ab[1].astype(F32)).astype(BF16)

    ab[0], ab[1] = gate_up(jnp.int32(0))
    refill_gu(jnp.int32(nr // 2))

    def mlp_step(f, _):
        a, b = gate_up(f)
        act(f - 1)
        ab[0] = a
        ab[1] = b

        @pl.when(f + nr // 2 < nf + no * nc // 2)
        def _():
            refill_gu(f + nr // 2)
        return 0

    lax.fori_loop(1, nf, mlp_step, 0)
    act(jnp.int32(nf - 1))

    def down_step(j, _):
        d = None
        for i in range(nc):
            m = j * nc + i
            down_copy(m).wait()
            part = jnp.dot(c_ref[:, i * d_model:(i + 1) * d_model], ring[lax.rem(no + 2 * nf + m, nr)],
                           preferred_element_type=F32)
            d = part if d is None else d + part
        out_ref[:, cols(j)] = (h1[:, cols(j)].astype(F32) + d.astype(BF16).astype(F32)).astype(BF16)
        return 0

    lax.fori_loop(0, no, down_step, 0)

    for g in range(groups):
        for step in (0, 1, 2, 4, 5, 6):
            for c in qkv_copies(g, step):
                c.wait_send()
        for off in range(1, n):
            o_copy(g, lax.rem(me + off, n)).wait_send()
    for off in range(1, n):
        seg_copy(lax.rem(me + off, n)).wait_send()


def decoder(n, hidden, seg_ids, g_kv, g_q, g_mlp, w_key, w_value, w_query, w_out, w_gate, w_up, w_down):
    tokens, d_model = hidden.shape
    _, q_heads, hd = w_query.shape
    heads = q_heads // n
    hw, pw, groups = heads * hd, 2 * hd, heads // 2
    tile, nr = 512, 18
    flat = lambda w: w.transpose(1, 2, 0).reshape(q_heads * hd, d_model)
    row = lambda g: g.reshape(1, d_model)
    vm = pl.BlockSpec(memory_space=pltpu.VMEM)
    hbm = pl.BlockSpec(memory_space=pl.ANY)
    dma = pltpu.SemaphoreType.DMA
    vb = lambda *s: pltpu.VMEM(s, BF16)
    kshape, tshape = (groups, n, tokens, pw), (groups, n, pw, tokens)
    return pl.pallas_call(
        functools.partial(kernel, n, heads, hd, tile, nr),
        out_shape=jax.ShapeDtypeStruct((tokens, d_model), BF16),
        in_specs=[vm] * 5 + [hbm] * 7,
        out_specs=vm,
        scratch_shapes=[
            vb(tokens, d_model), vb(tokens, d_model), vb(nr, d_model, tile),
            vb(groups, 6, tokens, pw), vb(groups, 6, pw, tokens), vb(groups, 6, pw, tokens), vb(*kshape), vb(*tshape), vb(*tshape),
            pltpu.VMEM((n, 1, tokens), jnp.int32), vb(n, tokens, 128), vb(n, 128, tokens),
            vb(*kshape), vb(tokens, n * hw),
            pltpu.VMEM((2, 2, tokens, tokens), F32), vb(2, 2, tokens, tokens),
            vb(2, tokens, tile), vb(tokens, w_gate.shape[1]),
            dma((3, 3, d_model // tile)), dma((nr,)), dma, dma, dma((groups, 3, 6)), dma((groups, 3, n)), dma((n,)), dma((n,)),
            dma((groups, n)), dma((groups, n)),
        ],
        compiler_params=pltpu.CompilerParams(collective_id=0, has_side_effects=True, vmem_limit_bytes=67043328),
    )(hidden, seg_ids.reshape(1, tokens), g_kv.reshape(d_model // 128, 128), row(g_q), row(g_mlp), flat(w_key), flat(w_query), flat(w_value),
      w_out.reshape(-1, d_model), w_gate, w_up, w_down)


def solution(mesh):
    n = mesh.shape['sp']

    def body(hidden, seg_ids, norm_kv, w_key, w_value, norm_attn, w_query, w_out, norm_mlp, w_gate, w_up, w_down):
        return decoder(n, hidden, seg_ids, norm_kv, norm_attn[0], norm_mlp[0], w_key, w_value, w_query[0], w_out[0],
                       w_gate[0], w_up[0], w_down[0])

    row_spec = P(('dp', 'sp'), None)
    in_specs = (row_spec, P(('dp', 'sp'))) + (P(),) * 10
    return jax.shard_map(body, mesh=mesh, in_specs=in_specs, out_specs=row_spec, check_vma=False)
```

```python
import functools
import jax
import jax.numpy as jnp
from jax import lax
from jax.experimental import pallas as pl
from jax.experimental.pallas import tpu as pltpu
from jax.sharding import PartitionSpec as P

NORM_EPS = 1e-6
MESH = pl.DeviceIdType.MESH
LOG2E = 1.4426950408889634
BIG = 2.0 ** 127
NT = (((1,), (1,)), ((), ()))
F32 = jnp.float32
BF16 = jnp.bfloat16


def route(me, n):
    chips = n // 2
    assert chips == 4
    chip, core = me // 2, lax.rem(me, 2)
    turn = 1 - 2 * core
    ahead = lax.rem(chip + turn + chips, chips) * 2
    behind = lax.rem(chip - turn + chips, chips) * 2
    return ahead, behind, chip * 2 + 1 - core, behind + core


def dest_of(me, n, step):
    ahead, behind, other, _ = route(me, n)
    pair = jnp.where(step < 4, behind, ahead) + lax.rem(step, 4)
    return jnp.where(lax.rem(step, 4) < 2, pair, jnp.where(lax.rem(step, 4) == 2, other, me))


def kernel(n, heads, hd, tile, nr, hid_ref, seg_ref, gkv_ref, gq_ref, gm_ref, wk_hbm, wq_hbm, wv_hbm,
           wo_hbm, wg_hbm, wu_hbm, wd_hbm, out_ref,
           ukv, uq, ring, ks, qs, vs, kr, qr, vr, segr, fk, fq, osend, orecv, s_scr, p_scr, ab, c_ref,
           wsem, sr, hand_ss, hand_rs, ssem, rsem, seg_ss, seg_rs, o_ss, o_rs):
    me = lax.axis_index('sp')
    tokens, d_model = hid_ref.shape
    ff = wg_hbm.shape[1]
    hw = heads * hd
    pw = 2 * hd
    groups = heads // 2
    nf = ff // tile
    no = d_model // tile

    def remote(s, d, ss, rs, p):
        return pltpu.make_async_remote_copy(s, d, ss, rs, device_id={'sp': p}, device_id_type=MESH)

    kp = d_model // tile
    nc = ff // d_model

    def wpieces(slot, i):
        b = slot * 3 + i
        per = tile // hw
        row = lax.rem(b, per) * kp * hw
        return [ring.at[nr - 5 + b // per, pl.ds(pl.multiple_of(row + k * hw, hw), hw)] for k in range(kp)]

    def wcopy(step):
        slot = lax.rem(step, 3)
        d = dest_of(me, n, step)
        rows = pl.ds(pl.multiple_of(d * hw, hw), hw)
        return [pltpu.make_async_copy(w.at[rows, k * tile:(k + 1) * tile], dst, wsem.at[slot, i, k])
                for i, w in enumerate((wk_hbm, wq_hbm, wv_hbm)) for k, dst in enumerate(wpieces(slot, i))]

    def cols(f):
        return pl.ds(pl.multiple_of(f * tile, tile), tile)

    def chunk(w, c, src):
        s = lax.rem(c, nr)
        return pltpu.make_async_copy(src, ring.at[s], sr.at[s])

    def out_copy(i):
        return chunk(wo_hbm, i, wo_hbm.at[:, cols(i)])

    def gate_copy(f):
        return chunk(wg_hbm, no + 2 * f, wg_hbm.at[:, cols(f)])

    def up_copy(f):
        return chunk(wu_hbm, no + 2 * f + 1, wu_hbm.at[:, cols(f)])

    def down_copy(m):
        rows = pl.ds(pl.multiple_of(lax.rem(m, nc) * d_model, d_model), d_model)
        return chunk(wd_hbm, no + 2 * nf + m, wd_hbm.at[rows, cols(m // nc)])

    def refill_gu(f):
        @pl.when(f < nf)
        def _():
            gate_copy(f).start()
            up_copy(f).start()

        @pl.when(f >= nf)
        def _():
            down_copy(2 * (f - nf)).start()
            down_copy(2 * (f - nf) + 1).start()

    for step in range(2):
        for c in wcopy(jnp.int32(step)):
            c.start()

    barrier = pltpu.get_barrier_semaphore()
    for off in range(1, n):
        pl.semaphore_signal(barrier, inc=1, device_id={'sp': lax.rem(me + off, n)}, device_id_type=MESH)

    def gain(ref):
        return jnp.concatenate([ref[i:i + 1].astype(F32) for i in range(d_model // 128)], axis=1)

    x = hid_ref[...].astype(F32)

    def normed(x):
        xn = x * lax.rsqrt(jnp.mean(x * x, axis=-1, keepdims=True) + NORM_EPS)
        return (xn * gain(gkv_ref)).astype(BF16), (xn * gq_ref[...].astype(F32)).astype(BF16)

    ukv[...], uq[...] = normed(x)
    segr[me] = seg_ref[...]

    def seg_copy(p):
        return remote(seg_ref, segr.at[me], seg_ss.at[p], seg_rs.at[me], p)

    ahead, _, _, origin = route(me, n)
    handed = c_ref.at[:, 0:d_model]
    y_kv = c_ref.at[:, d_model:2 * d_model]
    y_q = c_ref.at[:, 2 * d_model:3 * d_model]
    hand = remote(hid_ref, handed, hand_ss, hand_rs, ahead + lax.rem(me, 2))

    def qkv_copies(g, step):
        slot = step - step // 4
        shard = jnp.where(step < 4, me, origin)
        bufs = ((ks, kr), (qs, qr), (vs, vr))
        return [remote(s.at[g, slot], r.at[g, shard], ssem.at[g, i, slot], rsem.at[g, i, shard], dest_of(me, n, step))
                for i, (s, r) in enumerate(bufs)]

    def project(step, xkv, xq):
        for c in wcopy(step):
            c.wait()

        @pl.when(step + 2 < n)
        def _():
            for c in wcopy(step + 2):
                c.start()
        slot = lax.rem(step, 3)

        u_kv = [xkv[:, i * tile:(i + 1) * tile] for i in range(kp)]
        u_q = [xq[:, i * tile:(i + 1) * tile] for i in range(kp)]
        w = [[p[...] for p in wpieces(slot, i)] for i in range(3)]

        def nt(a, b):
            return sum(lax.dot_general(x, y, NT, preferred_element_type=F32) for x, y in zip(a, b)).astype(BF16)

        k, q, v = nt(u_kv, w[0]), nt(w[1], u_q), nt(w[2], u_kv)
        return k, q, v

    def store(step, xkv, xq):
        slot = step - step // 4
        k, q, v = project(step, xkv, xq)
        for g in range(groups):
            ks[g, slot] = k[:, g * pw:(g + 1) * pw]
            qs[g, slot] = q[g * pw:(g + 1) * pw]
            vs[g, slot] = v[g * pw:(g + 1) * pw]

    def keep(step, shard, xkv, xq):
        k, q, v = project(step, xkv, xq)
        for g in range(groups):
            kr[g, shard] = k[:, g * pw:(g + 1) * pw]
            qr[g, shard] = q[g * pw:(g + 1) * pw]
            vr[g, shard] = v[g * pw:(g + 1) * pw]

    def send(g, step):
        for c in qkv_copies(g, step):
            c.start()

    def own_step(step, _):
        store(step, ukv, uq)

        @pl.when(step == 0)
        def _():
            pl.semaphore_wait(barrier, n - 1)
            hand.start()
            for off in range(1, n):
                seg_copy(lax.rem(me + off, n)).start()
        return 0

    lax.fori_loop(0, 3, own_step, 0)
    for g in range(groups):
        send(g, 2)
    keep(jnp.int32(3), me, ukv, uq)
    lead = nr - 5
    for i in range(no):
        out_copy(i).start()
    for f in range((lead - no + 1) // 2):
        gate_copy(f).start()
        if no + 2 * f + 1 < lead:
            up_copy(f).start()
    hand.wait_send()
    for step in range(2):
        send(0, step)
    hand.wait_recv()
    y_kv[...], y_q[...] = normed(handed[...].astype(F32))

    def handed_step(step, _):
        store(step, y_kv, y_q)
        send(0, step)
        return 0

    lax.fori_loop(4, 6, handed_step, 0)
    for step in range(2):
        send(1, step)
    for g in range(1, groups):
        for step in (4, 5):
            send(g, step)
    lax.fori_loop(6, 7, handed_step, 0)
    for g in range(1, groups):
        send(g, 6)
    keep(jnp.int32(7), origin, y_kv, y_q)
    for c in range(lead, nr):
        (up_copy if (c - no) % 2 else gate_copy)((c - no) // 2).start()

    for off in range(1, n):
        p = lax.rem(me + off, n)
        remote(seg_ref, segr.at[p], seg_ss.at[p], seg_rs.at[p], p).wait_recv()
    ids = lax.broadcasted_iota(jnp.int32, (128, tokens), 0)

    def features(p, _):
        same = ids == segr[p]
        fq[p] = jnp.where(same, 1.0, 0.0).astype(BF16)
        fk[p] = jnp.where(same, 0.0, -BIG).T.astype(BF16)
        return 0

    lax.fori_loop(0, n, features, 0)

    scale = (hd ** -0.5) * LOG2E
    kpos = lax.broadcasted_iota(jnp.int32, (tokens, tokens), 0)
    qpos = lax.broadcasted_iota(jnp.int32, (tokens, tokens), 1)
    zero = jnp.zeros((hd, tokens), BF16)
    ones = jnp.ones((16, tokens), BF16)
    half = n // 2
    low = jnp.minimum(me, n - 1 - me)

    def o_cols(d, g):
        return orecv.at[:, pl.ds(pl.multiple_of(d * hw + g * pw, pw), pw)]

    def o_copy(g, j):
        return remote(osend.at[g, j], o_cols(me, g), o_ss.at[g, j], o_rs.at[g, me], j)

    def attend(g, j1):
        j2 = n - 1 - j1

        def q_ext(j):
            return (jnp.concatenate([qr[g, j, 0:hd], zero, fq[j]], axis=0),
                    jnp.concatenate([zero, qr[g, j, hd:pw], fq[j]], axis=0))

        qa, qb = q_ext(j1), q_ext(j2)

        def block(t):
            if t < 2:
                return (j1, j2)[t], t == 0
            first = t - 2 < j1
            return jnp.where(first, j1 + 1 - t, n - t), first

        def scores(t):
            i, first = block(t)
            kx = jnp.concatenate([kr[g, i], fk[i]], axis=1)
            for h in range(2):
                if t < 2:
                    q = (qa, qb)[t][h]
                else:
                    q = qb[h] if t > half else jnp.where(first, qa[h], qb[h])
                s_scr[t % 2, h] = jnp.dot(kx, q, preferred_element_type=F32)

        m_a, m_b, m = [None] * 2, [None] * 2, [None] * 2
        acc_a, acc_b, acc = [None] * 2, [None] * 2, [None] * 2
        alpha = {}

        def soft(t):
            for h in range(2):
                s = s_scr[t % 2, h]
                if t < 2:
                    s = jnp.where(kpos <= qpos, s, -BIG)
                    new = jnp.max(s, axis=0, keepdims=True)
                    (m_a, m_b)[t][h] = new
                else:
                    old = m_a[h] if t == 2 else m[h]
                    if t - 2 < half:
                        old = jnp.where(t - 2 == j1, m_b[h], old)
                    new = jnp.maximum(old, jnp.max(s, axis=0, keepdims=True))
                    alpha[t, h] = jnp.exp2((old - new) * scale)
                    m[h] = new
                p_scr[t % 2, h] = jnp.exp2((s - new) * scale).astype(BF16)

        def mix(t):
            i, _ = block(t)
            for h in range(2):
                vx = jnp.concatenate([vr[g, i, h * hd:(h + 1) * hd], ones], axis=0)
                d = jnp.dot(vx, p_scr[t % 2, h], preferred_element_type=F32)
                if t == 0:
                    acc[h] = d
                elif t == 1:
                    acc_b[h] = d
                else:
                    if t - 2 < half:
                        swap = t - 2 == j1
                        acc_a[h] = acc[h] if t == 2 else jnp.where(swap, acc[h], acc_a[h])
                        acc[h] = jnp.where(swap, acc_b[h], acc[h])
                    acc[h] = acc[h] * alpha[t, h] + d

        scores(0)
        for t in range(n + 2):
            if t < n:
                scores(t + 1)
            if t < n + 1:
                soft(t)
            if t >= 1:
                mix(t - 1)
        return [jnp.concatenate([r[h][0:hd] / r[h][hd:hd + 1] for h in range(2)], axis=0).T.astype(BF16)
                for r in (acc_a, acc)]

    def group(g, _):
        for off in range(1, n):
            p = lax.rem(me + off, n)

            @pl.when(p != origin)
            def _():
                for i, r in enumerate((kr, qr, vr)):
                    remote(r.at[g, p], r.at[g, p], ssem.at[g, i, 0], rsem.at[g, i, p], p).wait_recv()

        def unit(t, _):
            j1 = lax.rem(low + 1 + t, half)
            for j, o in zip((j1, n - 1 - j1), attend(g, j1)):
                osend[g, j] = o

                @pl.when(j != me)
                def _():
                    o_copy(g, j).start()
            return 0

        lax.fori_loop(0, half, unit, 0)
        orecv[:, pl.ds(pl.multiple_of(me * hw + g * pw, pw), pw)] = osend[g, me]
        return 0

    lax.fori_loop(0, groups, group, 0)

    for g in range(groups):
        for off in range(1, n):
            p = lax.rem(me + off, n)
            remote(osend.at[g, p], o_cols(p, g), o_ss.at[g, p], o_rs.at[g, p], p).wait_recv()

    h1, u = uq, ukv
    ssq = jnp.zeros((tokens, 1), F32)
    for i in range(no):
        out_copy(i).wait()
    for i in range(no):
        a = jnp.dot(orecv[...], ring[i], preferred_element_type=F32).astype(BF16)
        s = pl.ds(i * tile, tile)
        h = (hid_ref[:, s].astype(F32) + a.astype(F32)).astype(BF16)
        h1[:, s] = h
        h = h.astype(F32)
        ssq += jnp.sum(h * h, axis=-1, keepdims=True)
    for i in range(no // 2):
        refill_gu(jnp.int32((nr - no) // 2 + i))
    inv = lax.rsqrt(ssq / d_model + NORM_EPS)
    u[...] = (h1[...].astype(F32) * inv * gm_ref[...].astype(F32)).astype(BF16)

    def gate_up(f):
        for i in range(2):
            gate_copy(f + i).wait()
            up_copy(f + i).wait()
        out = []
        for i in range(2):
            s = lax.rem(no + 2 * (f + i), nr)
            out += [jnp.dot(u[...], ring[s + k], preferred_element_type=F32).astype(BF16) for k in range(2)]
        return out

    def act(f):
        for i in range(2):
            a = ab[2 * i].astype(F32)
            c_ref[:, cols(f + i)] = (jax.nn.silu(a) * ab[2 * i + 1].astype(F32)).astype(BF16)

    def keep_ab(v):
        for i in range(4):
            ab[i] = v[i]

    keep_ab(gate_up(jnp.int32(0)))
    for i in range(2):
        refill_gu(jnp.int32(nr // 2 + i))

    def mlp_step(t, _):
        f = 2 * t
        v = gate_up(f)
        act(f - 2)
        keep_ab(v)
        for i in range(2):
            @pl.when(f + i + nr // 2 < nf + no * nc // 2)
            def _():
                refill_gu(f + i + nr // 2)
        return 0

    lax.fori_loop(1, nf // 2, mlp_step, 0)
    act(jnp.int32(nf - 2))

    def down_step(j, _):
        d = None
        for i in range(nc):
            down_copy(j * nc + i).wait()
        for i in range(nc):
            m = j * nc + i
            part = jnp.dot(c_ref[:, i * d_model:(i + 1) * d_model], ring[lax.rem(no + 2 * nf + m, nr)],
                           preferred_element_type=F32)
            d = part if d is None else d + part
        out_ref[:, cols(j)] = (h1[:, cols(j)].astype(F32) + d.astype(BF16).astype(F32)).astype(BF16)
        return 0

    lax.fori_loop(0, no, down_step, 0)

    for g in range(groups):
        for step in (0, 1, 2, 4, 5, 6):
            for c in qkv_copies(g, step):
                c.wait_send()
        for off in range(1, n):
            o_copy(g, lax.rem(me + off, n)).wait_send()
    for off in range(1, n):
        seg_copy(lax.rem(me + off, n)).wait_send()


def decoder(n, hidden, seg_ids, g_kv, g_q, g_mlp, w_key, w_value, w_query, w_out, w_gate, w_up, w_down):
    tokens, d_model = hidden.shape
    _, q_heads, hd = w_query.shape
    heads = q_heads // n
    hw, pw, groups = heads * hd, 2 * hd, heads // 2
    tile, nr = 512, 18
    flat = lambda w: w.transpose(1, 2, 0).reshape(q_heads * hd, d_model)
    row = lambda g: g.reshape(1, d_model)
    vm = pl.BlockSpec(memory_space=pltpu.VMEM)
    hbm = pl.BlockSpec(memory_space=pl.ANY)
    dma = pltpu.SemaphoreType.DMA
    vb = lambda *s: pltpu.VMEM(s, BF16)
    kshape, tshape = (groups, n, tokens, pw), (groups, n, pw, tokens)
    return pl.pallas_call(
        functools.partial(kernel, n, heads, hd, tile, nr),
        out_shape=jax.ShapeDtypeStruct((tokens, d_model), BF16),
        in_specs=[vm] * 5 + [hbm] * 7,
        out_specs=vm,
        scratch_shapes=[
            vb(tokens, d_model), vb(tokens, d_model), vb(nr, d_model, tile),
            vb(groups, 6, tokens, pw), vb(groups, 6, pw, tokens), vb(groups, 6, pw, tokens), vb(*kshape), vb(*tshape), vb(*tshape),
            pltpu.VMEM((n, 1, tokens), jnp.int32), vb(n, tokens, 128), vb(n, 128, tokens),
            vb(*kshape), vb(tokens, n * hw),
            pltpu.VMEM((2, 2, tokens, tokens), F32), vb(2, 2, tokens, tokens),
            vb(4, tokens, tile), vb(tokens, w_gate.shape[1]),
            dma((3, 3, d_model // tile)), dma((nr,)), dma, dma, dma((groups, 3, 6)), dma((groups, 3, n)), dma((n,)), dma((n,)),
            dma((groups, n)), dma((groups, n)),
        ],
        compiler_params=pltpu.CompilerParams(collective_id=0, has_side_effects=True, vmem_limit_bytes=67043328),
    )(hidden, seg_ids.reshape(1, tokens), g_kv.reshape(d_model // 128, 128), row(g_q), row(g_mlp), flat(w_key), flat(w_query), flat(w_value),
      w_out.reshape(-1, d_model), w_gate, w_up, w_down)


def solution(mesh):
    n = mesh.shape['sp']

    def body(hidden, seg_ids, norm_kv, w_key, w_value, norm_attn, w_query, w_out, norm_mlp, w_gate, w_up, w_down):
        return decoder(n, hidden, seg_ids, norm_kv, norm_attn[0], norm_mlp[0], w_key, w_value, w_query[0], w_out[0],
                       w_gate[0], w_up[0], w_down[0])

    row_spec = P(('dp', 'sp'), None)
    in_specs = (row_spec, P(('dp', 'sp'))) + (P(),) * 10
    return jax.shard_map(body, mesh=mesh, in_specs=in_specs, out_specs=row_spec, check_vma=False)
```
